32 devices in a mesh: req: 16 (over z, y, x), tp: 2 (over core).
Axes of the slice: x: 2, y: 2, z: 4, core: 2. Of those that a mesh axis runs over, the one named last changes fastest.
Arguments:
- tree_queries: bfloat16 [16, 512, 4096], P('req', None, 'tp'), may hold values from -512 to 512
- tree_keys: bfloat16 [16, 512, 512], P('req', None, 'tp'), may hold values from -6 to 6
- tree_values: bfloat16 [16, 512, 512], P('req', None, 'tp'), may hold values from -6 to 6
- cache_keys: bfloat16 [16, 1024, 512], P('req', None, 'tp'), may hold values from -6 to 6
- cache_values: bfloat16 [16, 1024, 512], P('req', None, 'tp'), may hold values from -6 to 6
- sinks: float32 [64], P('tp'), may hold values from 7 to 11
- parents: int32 [16, 512], P('req'), may hold values from 0 to 510, as said below
- tile_counts: int32 [16], P('req'), may hold values from 1 to 4, 32 in all
- out_weight: bfloat16 [4096, 2880], P('tp', 'req'), may hold values from -0.71875 to 0.71875
Outputs:
- mixed: bfloat16 [16, 512, 2880], P('req', 'tp')
The draws below stay inside these ranges and needn't reach their ends.
Inputs may be any that keep to these rules, and one draw needn't show every extreme that they name: `parents`: each position's parent stands before it; position 0 is its own parent. `tile_counts`: the counts sum to 32.
All inputs are finite; a program needn't handle non-finite values. No bound on the sum of `tile_counts` on one device may be relied on, other than what follows from the above.
Results may differ from the reference program's by a relative error of at most 0.024.
Values may be sent and summed in bfloat16 or wider, within the bound.
No kernel may reach another device: no remote copies, remote signals or barrier semaphores. Data moves between devices by JAX's collectives and lax.ppermute only.
A program may use at most 128 MiB of HBM per device.

```python
import math
import jax
import jax.numpy as jnp
import numpy as np
from jax import lax

D = 2880
HEADS = 64
KV_HEADS = 8
HEAD_DIM = 64
TREE = 512
TILE = 128
CTX = 1024
REQS = 16
N_TP = 2


def shared_keys(key):
    array_shape = (REQS, CTX, KV_HEADS * HEAD_DIM)
    drawn = jnp.clip(jax.random.normal(jax.random.fold_in(key, 7), array_shape, jnp.float32), -6.0, 6.0)
    return drawn


def draw_cache_keys(key, part):
    return shared_keys(key).astype(jnp.bfloat16)


def draw_tree_queries(key, part):
    array_shape = (REQS, TREE, HEADS * HEAD_DIM)
    drawn = 2.0 * jnp.clip(jax.random.normal(jax.random.fold_in(key, 3), array_shape, jnp.float32), -6.0, 6.0)
    return drawn.astype(jnp.bfloat16)


def draw_parents(key, part):
    positions = jnp.arange(TREE, dtype=jnp.int32)
    chooser = jax.random.randint(jax.random.fold_in(key, 1), (REQS, TREE), 0, 10)
    anywhere = jax.random.randint(jax.random.fold_in(key, 2), (REQS, TREE), 0, TREE) % jnp.maximum(positions, 1)
    parent_row = jnp.where(chooser < 7, positions - 1, anywhere)
    return jnp.maximum(parent_row, 0).astype(jnp.int32)


def block_scale(key, dims, cuts, low, high):
    def one(dim, shards_of):
        draws = jax.random.uniform(jax.random.fold_in(jax.random.fold_in(key, 6), dim), (shards_of,), jnp.float32, low / len(cuts), high / len(cuts))
        return jnp.repeat(jnp.exp(draws), dims[dim] // shards_of).reshape((-1,) + (1,) * (len(dims) - dim - 1))

    gain = one(*cuts[0])
    for cut in cuts[1:]:
        gain = gain * one(*cut)
    return gain


def profile(amount, total, bound, slope):
    loads = [(1 << 20) // math.isqrt(grade ** slope) + 1 for grade in range(2, amount + 1)]
    rest, holding = total - bound - (amount - 1), [1] * (amount - 1)
    while rest > 0:
        candidates = [i for i in range(amount - 1) if holding[i] < bound]
        whole, remaining = sum([loads[i] for i in candidates]), rest
        for i in candidates:
            extra = min(bound - holding[i], max(1, remaining * loads[i] // whole), rest)
            holding[i] = holding[i] + extra
            rest = rest - extra
    return np.array([bound] + holding)


def ragged(key, count, total, reach, slope):
    if count == 2:
        one = jax.random.randint(key, (), max(1, total - reach), min(reach, total - 1) + 1)
        return jnp.stack([one, total - one])
    tallies = jnp.asarray(profile(count, total, reach, slope), jnp.int32)
    twos = (count - 1) // 2
    donor, sink = tallies[1:1 + 2 * twos:2], tallies[2:2 + 2 * twos:2]
    room = jnp.minimum(donor - 1, reach - sink)
    passed = jax.random.randint(jax.random.fold_in(key, 1), (twos,), 0, 1 << 20) % (room + 1)
    tallies = tallies.at[1:1 + 2 * twos:2].set(donor - passed).at[2:2 + 2 * twos:2].set(sink + passed)
    return tallies[jax.random.permutation(jax.random.fold_in(key, 2), count)]


def gaussian(own_key, extent, spread, bound, split=(), held_as=jnp.bfloat16):
    result = spread * jax.random.normal(own_key, extent, jnp.float32)
    if split:
        result = result * block_scale(own_key, extent, split, -0.22, 0.18)
    return jnp.clip(result, -bound, bound).astype(held_as)


def setup_inputs(seed: int = 0) -> dict:
    splits = jax.random.split(jax.random.key(seed), 10)
    return {
        "tree_queries": draw_tree_queries(jax.random.fold_in(splits[9], 71), 0),
        "tree_keys": gaussian(splits[1], (REQS, TREE, KV_HEADS * HEAD_DIM), 1.0, 6.0, ((0, 16), (2, 2))),
        "tree_values": gaussian(splits[2], (REQS, TREE, KV_HEADS * HEAD_DIM), 1.0, 6.0, ((0, 16), (2, 2))),
        "cache_keys": draw_cache_keys(jax.random.fold_in(splits[9], 71), 0),
        "cache_values": gaussian(splits[4], (REQS, CTX, KV_HEADS * HEAD_DIM), 1.0, 6.0, ((0, 16), (2, 2))),
        "sinks": jnp.clip(7.0 + 4.0 * jax.random.uniform(splits[5], (HEADS,), jnp.float32) ** block_scale(splits[5], (HEADS,), ((0, 2),), -0.2, 0.2), 7.0, 11.0),
        "parents": draw_parents(jax.random.fold_in(splits[9], 71), 0),
        "tile_counts": ragged(splits[7], REQS, 2 * REQS, TREE // TILE, 2).astype(jnp.int32),
        "out_weight": gaussian(splits[8], (HEADS * HEAD_DIM, D), 0.12, 0.71875, ((0, 2), (1, 16))),
    }


masked_score = -1e30


def ancestry(parents):
    length = parents.shape[0]
    upward = parents
    visible = jnp.eye(length, dtype=jnp.int32)
    doubling = 0
    while (1 << doubling) < length:
        visible = jnp.maximum(visible, jnp.take(visible, upward, axis=0))
        upward = jnp.take(upward, upward, axis=0)
        doubling += 1
    return visible


def request_attention(queries, tree_keys, tree_values, cache_keys, cache_values, sinks, parents, live_tiles):
    group_size = HEADS // KV_HEADS
    visible = ancestry(parents)
    scaling = HEAD_DIM ** -0.5
    query_heads = queries.astype(jnp.float32).reshape(TREE, KV_HEADS, group_size, HEAD_DIM).transpose(1, 0, 2, 3)
    all_keys = jnp.concatenate([cache_keys, tree_keys], 0).astype(jnp.float32).reshape(CTX + TREE, KV_HEADS, HEAD_DIM).transpose(1, 0, 2)
    all_values = jnp.concatenate([cache_values, tree_values], 0).astype(jnp.float32).reshape(CTX + TREE, KV_HEADS, HEAD_DIM).transpose(1, 0, 2)
    allowed = jnp.concatenate([jnp.ones((TREE, CTX), dtype=jnp.int32), visible], 1) > 0
    sink_heads = sinks.reshape(KV_HEADS, group_size)

    def per_head(operands):
        query_block, key_block, value_block, sink_row = operands
        scores = jnp.einsum("tgd,cd->gtc", query_block, key_block) * scaling
        scores = jnp.where(allowed[None], scores, masked_score)
        maxima = jnp.maximum(scores.max(-1), sink_row[:, None])
        weights = jnp.exp(scores - maxima[..., None])
        denominator = weights.sum(-1) + jnp.exp(sink_row[:, None] - maxima)
        rounded = weights.astype(jnp.bfloat16).astype(jnp.float32)
        weighted = jnp.einsum("gtc,cd->gtd", rounded, value_block)
        return weighted / denominator[..., None]

    per_heads = lax.map(per_head, (query_heads, all_keys, all_values, sink_heads))
    attention = per_heads.transpose(2, 0, 1, 3).reshape(TREE, HEADS * HEAD_DIM)
    live_rows = jnp.arange(TREE, dtype=jnp.int32) < live_tiles * TILE
    return jnp.where(live_rows[:, None], attention, 0.0).astype(jnp.bfloat16)


def reference(tree_queries, tree_keys, tree_values, cache_keys, cache_values, sinks, parents, tile_counts, out_weight):
    weight_groups = out_weight.astype(jnp.float32).reshape(N_TP, HEADS * HEAD_DIM // N_TP, D)

    def per_request(operands):
        queries, keys_tree, values_tree, keys_cache, values_cache, parent_row, live_tiles = operands
        attention = request_attention(queries, keys_tree, values_tree, keys_cache, values_cache, sinks, parent_row, live_tiles)
        pieces = attention.astype(jnp.float32).reshape(TREE, N_TP, HEADS * HEAD_DIM // N_TP)
        partial_value = jnp.einsum("tnh,nhd->ntd", pieces, weight_groups).astype(jnp.bfloat16)
        partial_value = lax.optimization_barrier(partial_value)
        return partial_value.astype(jnp.float32).sum(0).astype(jnp.bfloat16)

    return lax.map(per_request, (tree_queries, tree_keys, tree_values, cache_keys, cache_values, parents, tile_counts))
```

```python
import functools

import jax
import jax.numpy as jnp
from jax import lax
from jax.experimental import pallas as pl
from jax.experimental.pallas import tpu as pltpu
from jax.sharding import PartitionSpec as P


HEADS = 64
KV_HEADS = 8
HEAD_DIM = 64
TREE = 512
TILE = 128
WIDE = 2 * HEAD_DIM
LOG2_E = 1.4426950408889634
masked_score = -1e30


def product(left, right):
    return jnp.dot(left, right, preferred_element_type=jnp.float32)


def ancestry_kernel(parent_ref, bias_ref, seen):
    tiles = TREE // TILE
    lane = lax.broadcasted_iota(jnp.int32, (TILE, TILE), 1)
    key = lax.broadcasted_iota(jnp.int32, (TILE, TILE), 0)

    def hop(key_tile, row_tile):
        parent = parent_ref[:, row_tile * TILE : (row_tile + 1) * TILE]
        return jnp.broadcast_to(parent, (TILE, TILE)) == key + key_tile * TILE

    inner = [(hop(t, t) | (lane == key)).astype(jnp.bfloat16) for t in range(tiles)]
    reach = 1
    while reach < TILE:
        inner = [jnp.minimum(product(r, r), 1.0).astype(jnp.bfloat16) for r in inner]
        reach *= 2
    seen[...] = jnp.zeros_like(seen)
    for t in range(tiles):
        rows = slice(t * TILE, (t + 1) * TILE)
        if t:
            up = jnp.concatenate([hop(u, t).astype(jnp.bfloat16) for u in range(t)], 0)
            last = product(up, inner[t]).astype(jnp.bfloat16)
            seen[: t * TILE, rows] = product(seen[: t * TILE, : t * TILE], last).astype(jnp.bfloat16)
        seen[rows, rows] = inner[t]
    bias_ref[...] = jnp.where(seen[...].astype(jnp.float32) > 0.5, 0.0, masked_score)


def ancestry(parents):
    return pl.pallas_call(
        ancestry_kernel,
        out_shape=jax.ShapeDtypeStruct((TREE, TREE), jnp.float32),
        in_specs=[pl.BlockSpec(memory_space=pltpu.VMEM)],
        out_specs=pl.BlockSpec(memory_space=pltpu.VMEM),
        scratch_shapes=[pltpu.VMEM((TREE, TREE), jnp.bfloat16)],
        compiler_params=pltpu.CompilerParams(vmem_limit_bytes=8 << 20),
        name="ancestry",
        cost_estimate=pl.CostEstimate(
            flops=2 * TREE**3, bytes_accessed=4 * TREE * TREE, transcendentals=0
        ),
    )(parents)


ONES = 16


def attend_kernel(
    kv_head,
    first,
    live_ref,
    sink_ref,
    query_ref,
    tree_k_ref,
    tree_v_ref,
    cache_k_ref,
    cache_v_ref,
    bias_ref,
    out_ref,
    key_left,
    key_right,
    values,
    score_left,
    score_right,
):
    ctx = cache_k_ref.shape[0]
    pairs = out_ref.shape[0] // WIDE
    factor = LOG2_E * HEAD_DIM**-0.5
    sink_scale = HEAD_DIM**0.5
    near = kv_head % 2
    columns = slice(kv_head // 2 * WIDE, kv_head // 2 * WIDE + WIDE)
    for start, key_src, value_src in (
        (0, cache_k_ref, cache_v_ref),
        (ctx, tree_k_ref, tree_v_ref),
    ):
        rows = key_src.shape[0]
        span = slice(start, start + rows)
        right = lax.broadcasted_iota(jnp.int32, (rows, WIDE), 1) >= HEAD_DIM
        own = right if near else jnp.logical_not(right)
        key = jnp.where(own, key_src[:, columns].astype(jnp.float32), 0.0)
        moved = pltpu.roll(key, HEAD_DIM, 1)
        key_left[span] = (moved if near else key).astype(jnp.bfloat16)
        key_right[span] = (key if near else moved).astype(jnp.bfloat16)
        turned = value_src[:, columns].astype(jnp.float32).T
        values[:HEAD_DIM, span] = turned[near * HEAD_DIM : (near + 1) * HEAD_DIM].astype(jnp.bfloat16)
    values[HEAD_DIM:] = jnp.ones((ONES, values.shape[1]), jnp.bfloat16)
    live = live_ref[0]

    def score(tile, keys, store):
        rows = pl.ds(pl.multiple_of(tile * TILE, TILE), TILE)
        start = first * HEAD_DIM
        query = jnp.concatenate(
            [query_ref[rows, start + p * WIDE : start + (p + 1) * WIDE] for p in range(pairs)], 0
        )
        store[...] = lax.dot_general(
            keys[...], query, (((1,), (1,)), ((), ())), preferred_element_type=jnp.float32
        )

    def mix(tile, side, store):
        rows = pl.ds(pl.multiple_of(tile * TILE, TILE), TILE)
        bias = bias_ref[:, rows]
        bias = jnp.concatenate([bias] * pairs, 1)
        scores = jnp.concatenate([store[:ctx], store[ctx:] + bias], 0)
        sinks = [sink_ref[:, first + 2 * p + side : first + 2 * p + side + 1] for p in range(pairs)]
        sink = jnp.concatenate([jnp.broadcast_to(s, (1, TILE)) for s in sinks], 1) * sink_scale
        peak = jnp.maximum(scores.max(0, keepdims=True), sink)
        probs = jnp.exp2((scores - peak) * factor).astype(jnp.bfloat16)
        sums = product(values[...], probs)
        below = sums[HEAD_DIM : HEAD_DIM + 1] + jnp.exp2((sink - peak) * factor)
        mixed = (sums[:HEAD_DIM] / below).astype(out_ref.dtype)
        for p in range(pairs):
            top = p * WIDE + side * HEAD_DIM
            out_ref[top : top + HEAD_DIM, rows] = mixed[:, p * TILE : (p + 1) * TILE]

    out_ref[...] = jnp.zeros_like(out_ref)
    score(0, key_left, score_left)

    @pl.loop(0, live)
    def tile_step(tile):
        score(tile, key_right, score_right)
        mix(tile, 0, score_left)
        score(jnp.minimum(tile + 1, live - 1), key_left, score_left)
        mix(tile, 1, score_right)


def attend(part, parts, live, sinks, queries, tree_k, tree_v, cache_k, cache_v, bias):
    width = queries.shape[1] // parts
    first = part * width // HEAD_DIM
    kv_head = first // (HEADS // KV_HEADS)
    keys = cache_k.shape[0] + tree_k.shape[0]
    smem = pl.BlockSpec(memory_space=pltpu.SMEM)
    vmem = pl.BlockSpec(memory_space=pltpu.VMEM)
    rows = width // WIDE * TILE
    return pl.pallas_call(
        functools.partial(attend_kernel, kv_head, first),
        out_shape=jax.ShapeDtypeStruct((width, TREE), jnp.bfloat16),
        in_specs=[smem] + [vmem] * 7,
        out_specs=vmem,
        scratch_shapes=[
            pltpu.VMEM((keys, WIDE), jnp.bfloat16),
            pltpu.VMEM((keys, WIDE), jnp.bfloat16),
            pltpu.VMEM((HEAD_DIM + ONES, keys), jnp.bfloat16),
            pltpu.VMEM((keys, rows), jnp.float32),
            pltpu.VMEM((keys, rows), jnp.float32),
        ],
        compiler_params=pltpu.CompilerParams(vmem_limit_bytes=16 << 20),
        cost_estimate=pl.CostEstimate(
            flops=16 * TREE * keys * width, bytes_accessed=3 << 20, transcendentals=0
        ),
    )(live, sinks, queries, tree_k, tree_v, cache_k, cache_v, bias)


def project_kernel(line, parts, ranks, whom_ref, *refs):
    blocks = sum(len(candidates) for candidates in line)
    weights, refs = refs[:blocks], refs[blocks:]
    requests, outs, (held, sems) = refs[: 2 * parts], refs[2 * parts : -2], refs[-2:]
    place, rank = whom_ref[0] // 4, whom_ref[1]
    offset = 0
    for n, candidates in enumerate(line):
        for i, places in enumerate(candidates):
            copy = pltpu.make_async_copy(weights[offset + i], held.at[n], sems.at[n])
            if len(candidates) == 1:
                copy.start()
            else:
                here = functools.reduce(jnp.logical_or, [place == p for p in places])
                pl.when(here)(copy.start)
        offset += len(candidates)
    rows = outs[0].shape[-1]
    for n in range(len(line)):
        pltpu.make_async_copy(weights[0], held.at[n], sems.at[n]).wait()
        for which in range(2):
            for shift, out_ref in enumerate(outs):
                span = slice(None)
                if len(outs) > 1:
                    span = pl.ds(pl.multiple_of((rank + shift) % ranks * rows, rows), rows)
                total = 0.0
                for part in range(parts):
                    attention = requests[which * parts + part]
                    depth = attention.shape[0]
                    lanes = slice(part * depth, (part + 1) * depth)
                    total = total + product(held[n, :, lanes], attention[:, span])
                out_ref[which, n] = total.astype(out_ref.dtype)


def project(whom, ranks, line, own, partner):
    blocks = [block for candidates in line for block, _ in candidates]
    columns, depth = blocks[0].shape
    count = len(line)
    rows = TREE // ranks
    cut = rows % 128 == 0
    shape = (2, count, columns, rows if cut else TREE)
    vmem = pl.BlockSpec(memory_space=pltpu.VMEM)
    outs = pl.pallas_call(
        functools.partial(
            project_kernel, [[p for _, p in candidates] for candidates in line], len(own), ranks
        ),
        out_shape=[jax.ShapeDtypeStruct(shape, jnp.bfloat16)] * (ranks if cut else 1),
        in_specs=[pl.BlockSpec(memory_space=pltpu.SMEM)]
        + [pl.BlockSpec(memory_space=pl.ANY)] * len(blocks)
        + [vmem] * (2 * len(own)),
        out_specs=[vmem] * (ranks if cut else 1),
        scratch_shapes=[
            pltpu.VMEM((count, columns, depth), jnp.bfloat16),
            pltpu.SemaphoreType.DMA((count,)),
        ],
        compiler_params=pltpu.CompilerParams(vmem_limit_bytes=16 << 20),
        cost_estimate=pl.CostEstimate(
            flops=8 * count * columns * depth * TREE,
            bytes_accessed=2 * count * columns * (depth + 2 * TREE),
            transcendentals=0,
        ),
    )(whom, *blocks, *own, *partner)
    if cut:
        return list(outs)
    rank = whom[1]
    return [
        lax.dynamic_slice_in_dim(outs[0], (rank + shift) % ranks * rows, rows, 3)
        for shift in range(ranks)
    ]


def settle_kernel(count, *refs):
    for which in range(2):
        total = refs[0][which].astype(jnp.float32)
        for term in refs[1:count]:
            total = total + term[which].astype(jnp.float32)
        refs[count + which][...] = total.astype(jnp.bfloat16)


def settle(terms):
    vmem = pl.BlockSpec(memory_space=pltpu.VMEM)
    shape = jax.ShapeDtypeStruct(terms[0].shape[1:], jnp.bfloat16)
    return pl.pallas_call(
        functools.partial(settle_kernel, len(terms)),
        out_shape=[shape] * 2,
        in_specs=[vmem] * len(terms),
        out_specs=[vmem] * 2,
        compiler_params=pltpu.CompilerParams(vmem_limit_bytes=16 << 20),
    )(*terms)


def arrange_kernel(homes, groups, whom_ref, *refs):
    parts, (out_ref, held) = refs[: 2 * groups], refs[2 * groups :]
    request = whom_ref[0]
    place, side, member = request // 4, request // 2 % 2, request % 2
    slots = len(homes[0]) * 2
    for which in range(2):
        at = 0
        for part in parts[which * groups : (which + 1) * groups]:
            held[which * slots + at : which * slots + at + part.shape[0]] = part[...]
            at += part.shape[0]
    columns = held.shape[1]

    def block(index):
        slot = 0
        for p, row in enumerate(homes):
            slot = jnp.where(place == p, row[index // 4], slot)
        slot = slot * 2 + jnp.where(side == index // 2 % 2, 0, 1)
        return held[slot + jnp.where(member == index % 2, 0, slots)].astype(jnp.float32)

    for pair in range(slots):
        both = jnp.concatenate([block(2 * pair), block(2 * pair + 1)], 0)
        out_ref[2 * pair * columns : 2 * (pair + 1) * columns] = both.astype(out_ref.dtype)


def arrange(whom, homes, mine, other):
    vmem = pl.BlockSpec(memory_space=pltpu.VMEM)
    columns, rows = mine[0].shape[1:]
    count = sum(part.shape[0] for part in mine + other)
    return pl.pallas_call(
        functools.partial(arrange_kernel, homes, len(mine)),
        out_shape=jax.ShapeDtypeStruct((count * columns, rows), jnp.bfloat16),
        in_specs=[pl.BlockSpec(memory_space=pltpu.SMEM)] + [vmem] * (2 * len(mine)),
        out_specs=vmem,
        scratch_shapes=[pltpu.VMEM((count, columns, rows), jnp.bfloat16)],
        compiler_params=pltpu.CompilerParams(vmem_limit_bytes=16 << 20),
        name="arrange",
    )(whom, *mine, *other)


def arrivals(place, length):
    below = [(place - step, "up", step) for step in range(1, place + 1)]
    above = [(place + step, "down", step) for step in range(1, length - place)]
    return sorted(below + above, key=lambda item: (item[2], item[1] == "down"))


def timetable(length, parts):
    plan = {}
    at = 2
    for step in range(1, length):
        plan.setdefault(min(at, parts), []).append(("face", step))
        if step + 1 < length:
            plan.setdefault(min(at + 1, parts), []).append(("line", step + 1))
        at += 3
    return plan


def per_device(
    reqs,
    ranks,
    tree_queries,
    tree_keys,
    tree_values,
    cache_keys,
    cache_values,
    sinks,
    parents,
    tile_counts,
    out_weight,
):
    length = reqs // 4
    whom = jnp.stack([lax.axis_index("req"), lax.axis_index("tp")]).astype(jnp.int32)
    order = [arrivals(p, length) for p in range(length)]

    def along(step):
        return [
            (p * 4 + low, (p + step) * 4 + low)
            for p in range(length)
            for low in range(4)
            if 0 <= p + step < length
        ]

    def restrict(hops, keep):
        return [hop for hop in hops if keep(hop[0] // 4)]

    across = [(i, i ^ 2) for i in range(reqs)]
    swap = [(i, i ^ 1) for i in range(reqs)]
    columns = out_weight.T
    line = {("up", 0): columns, ("down", 0): columns}
    facing = {("up", 0): lax.ppermute(columns, "req", across)}

    def forward(kind, step):
        for way, sign in (("up", 1), ("down", -1)):
            if kind == "face":
                hops = restrict(across, lambda p: 0 <= p - sign * step < length)
                facing[way, step] = lax.ppermute(line[way, step], "req", hops)
                continue

            def sends(p):
                return 0 <= p - sign * (step - 1) < length and 0 <= p + sign < length

            hops = restrict(along(sign), sends)
            line[way, step] = lax.ppermute(line[way, step - 1], "req", hops)

    kv_local = cache_keys.shape[2] // HEAD_DIM
    odd = kv_local % 2 * HEAD_DIM
    tree_k, tree_v, cache_k, cache_v = (
        jnp.pad(array[0], ((0, 0), (0, odd)))
        for array in (tree_keys, tree_values, cache_keys, cache_values)
    )
    forward("line", 1)
    bias = ancestry(parents)
    own, partner = [], []
    parts = 2 * kv_local
    plan = timetable(length, parts)
    live = tile_counts
    for part in range(parts + 1):
        for kind, step in plan.get(part, []):
            if part < parts:
                needed = step if kind == "face" else step - 1
                live, *_ = lax.optimization_barrier((live, line["up", needed], line["down", needed]))
            forward(kind, step)
        if part == parts:
            break
        chunk = attend(
            part,
            parts,
            live,
            sinks[None],
            tree_queries[0],
            tree_k,
            tree_v,
            cache_k,
            cache_v,
            bias,
        )
        live, chunk = lax.optimization_barrier((live, chunk))
        own.append(chunk)
        partner.append(lax.ppermute(chunk, "req", swap))

    table = [
        [(("up", 0), p)] + [((way, step), source) for source, way, step in order[p]]
        for p in range(length)
    ]
    homes = [[0] * length for _ in range(length)]
    for p, row in enumerate(table):
        for n, (_, source) in enumerate(row):
            homes[p][source] = n

    def candidates(store, n):
        keys = sorted({row[n][0] for row in table})
        return [(store[k], [p for p, row in enumerate(table) if row[n][0] == k]) for k in keys]

    slots = [(store, n) for n in range(length) for store in (line, facing)]
    groups = [g for g in (slots[:3], slots[3:-2], slots[-2:-1], slots[-1:]) if g]
    mine, other = [], []
    for group in groups:
        terms = project(whom, ranks, [candidates(*slot) for slot in group], own, partner)
        for shift in range(1, ranks):
            hops = [(r, (r + shift) % ranks) for r in range(ranks)]
            terms[shift] = lax.ppermute(terms[shift], "tp", hops)
        kept, given = settle(terms)
        mine.append(kept)
        other.append(lax.ppermute(given, "req", swap))
    return arrange(whom, homes, mine, other).T[None]


def solution(mesh):
    in_specs = (
        P("req", None, "tp"),
        P("req", None, "tp"),
        P("req", None, "tp"),
        P("req", None, "tp"),
        P("req", None, "tp"),
        P("tp"),
        P("req", None),
        P("req"),
        P("tp", "req"),
    )
    out_specs = P("req", "tp", None)
    return jax.shard_map(
        functools.partial(per_device, mesh.shape["req"], mesh.shape["tp"]),
        mesh=mesh,
        in_specs=in_specs,
        out_specs=out_specs,
        check_vma=False,
    )
```

```python
import functools

import jax
import jax.numpy as jnp
from jax import lax
from jax.experimental import pallas as pl
from jax.experimental.pallas import tpu as pltpu
from jax.sharding import PartitionSpec as P


HEADS = 64
KV_HEADS = 8
HEAD_DIM = 64
TREE = 512
TILE = 128
WIDE = 2 * HEAD_DIM
LOG2_E = 1.4426950408889634
masked_score = -1e30


def product(left, right):
    return jnp.dot(left, right, preferred_element_type=jnp.float32)


def ancestry_kernel(parent_ref, bias_ref, seen):
    tiles = TREE // TILE
    lane = lax.broadcasted_iota(jnp.int32, (TILE, TILE), 1)
    key = lax.broadcasted_iota(jnp.int32, (TILE, TILE), 0)

    def hop(key_tile, row_tile):
        parent = parent_ref[:, row_tile * TILE : (row_tile + 1) * TILE]
        return jnp.broadcast_to(parent, (TILE, TILE)) == key + key_tile * TILE

    inner = [(hop(t, t) | (lane == key)).astype(jnp.bfloat16) for t in range(tiles)]
    reach = 1
    while reach < TILE:
        inner = [jnp.minimum(product(r, r), 1.0).astype(jnp.bfloat16) for r in inner]
        reach *= 2
    seen[...] = jnp.zeros_like(seen)
    for t in range(tiles):
        rows = slice(t * TILE, (t + 1) * TILE)
        if t:
            up = jnp.concatenate([hop(u, t).astype(jnp.bfloat16) for u in range(t)], 0)
            last = product(up, inner[t]).astype(jnp.bfloat16)
            seen[: t * TILE, rows] = product(seen[: t * TILE, : t * TILE], last).astype(jnp.bfloat16)
        seen[rows, rows] = inner[t]
    bias_ref[...] = jnp.where(seen[...].astype(jnp.float32) > 0.5, 0.0, masked_score)


def ancestry(parents):
    return pl.pallas_call(
        ancestry_kernel,
        out_shape=jax.ShapeDtypeStruct((TREE, TREE), jnp.float32),
        in_specs=[pl.BlockSpec(memory_space=pltpu.VMEM)],
        out_specs=pl.BlockSpec(memory_space=pltpu.VMEM),
        scratch_shapes=[pltpu.VMEM((TREE, TREE), jnp.bfloat16)],
        compiler_params=pltpu.CompilerParams(vmem_limit_bytes=8 << 20),
        name="ancestry",
        cost_estimate=pl.CostEstimate(
            flops=80 * TREE**3, bytes_accessed=4 * TREE * TREE, transcendentals=0
        ),
    )(parents)


ONES = 16


def attend_kernel(
    kv_head,
    first,
    live_ref,
    sink_ref,
    query_ref,
    tree_k_ref,
    tree_v_ref,
    cache_k_ref,
    cache_v_ref,
    bias_ref,
    out_ref,
    key_left,
    key_right,
    values,
    score_left,
    score_right,
):
    ctx = cache_k_ref.shape[0]
    pairs = out_ref.shape[0] // WIDE
    factor = LOG2_E * HEAD_DIM**-0.5
    sink_scale = HEAD_DIM**0.5
    near = kv_head % 2
    columns = slice(kv_head // 2 * WIDE, kv_head // 2 * WIDE + WIDE)
    for start, key_src, value_src in (
        (0, cache_k_ref, cache_v_ref),
        (ctx, tree_k_ref, tree_v_ref),
    ):
        rows = key_src.shape[0]
        span = slice(start, start + rows)
        right = lax.broadcasted_iota(jnp.int32, (rows, WIDE), 1) >= HEAD_DIM
        own = right if near else jnp.logical_not(right)
        key = jnp.where(own, key_src[:, columns].astype(jnp.float32), 0.0)
        moved = pltpu.roll(key, HEAD_DIM, 1)
        key_left[span] = (moved if near else key).astype(jnp.bfloat16)
        key_right[span] = (key if near else moved).astype(jnp.bfloat16)
        turned = value_src[:, columns].astype(jnp.float32).T
        values[:HEAD_DIM, span] = turned[near * HEAD_DIM : (near + 1) * HEAD_DIM].astype(jnp.bfloat16)
    values[HEAD_DIM:] = jnp.ones((ONES, values.shape[1]), jnp.bfloat16)
    live = live_ref[0]

    def score(tile, keys, store):
        rows = pl.ds(pl.multiple_of(tile * TILE, TILE), TILE)
        start = first * HEAD_DIM
        query = jnp.concatenate(
            [query_ref[rows, start + p * WIDE : start + (p + 1) * WIDE] for p in range(pairs)], 0
        )
        store[...] = lax.dot_general(
            keys[...], query, (((1,), (1,)), ((), ())), preferred_element_type=jnp.float32
        )

    def mix(tile, side, store):
        rows = pl.ds(pl.multiple_of(tile * TILE, TILE), TILE)
        bias = bias_ref[:, rows]
        bias = jnp.concatenate([bias] * pairs, 1)
        scores = jnp.concatenate([store[:ctx], store[ctx:] + bias], 0)
        sinks = [sink_ref[:, first + 2 * p + side : first + 2 * p + side + 1] for p in range(pairs)]
        sink = jnp.concatenate([jnp.broadcast_to(s, (1, TILE)) for s in sinks], 1) * sink_scale
        peak = jnp.maximum(scores.max(0, keepdims=True), sink)
        probs = jnp.exp2((scores - peak) * factor).astype(jnp.bfloat16)
        sums = product(values[...], probs)
        below = sums[HEAD_DIM : HEAD_DIM + 1] + jnp.exp2((sink - peak) * factor)
        mixed = (sums[:HEAD_DIM] / below).astype(out_ref.dtype)
        for p in range(pairs):
            top = p * WIDE + side * HEAD_DIM
            out_ref[top : top + HEAD_DIM, rows] = mixed[:, p * TILE : (p + 1) * TILE]

    out_ref[...] = jnp.zeros_like(out_ref)
    score(0, key_left, score_left)

    @pl.loop(0, live)
    def tile_step(tile):
        score(tile, key_right, score_right)
        mix(tile, 0, score_left)
        score(jnp.minimum(tile + 1, live - 1), key_left, score_left)
        mix(tile, 1, score_right)


def attend(part, parts, live, sinks, queries, tree_k, tree_v, cache_k, cache_v, bias):
    width = queries.shape[1] // parts
    first = part * width // HEAD_DIM
    kv_head = first // (HEADS // KV_HEADS)
    keys = cache_k.shape[0] + tree_k.shape[0]
    smem = pl.BlockSpec(memory_space=pltpu.SMEM)
    vmem = pl.BlockSpec(memory_space=pltpu.VMEM)
    rows = width // WIDE * TILE
    return pl.pallas_call(
        functools.partial(attend_kernel, kv_head, first),
        out_shape=jax.ShapeDtypeStruct((width, TREE), jnp.bfloat16),
        in_specs=[smem] + [vmem] * 7,
        out_specs=vmem,
        scratch_shapes=[
            pltpu.VMEM((keys, WIDE), jnp.bfloat16),
            pltpu.VMEM((keys, WIDE), jnp.bfloat16),
            pltpu.VMEM((HEAD_DIM + ONES, keys), jnp.bfloat16),
            pltpu.VMEM((keys, rows), jnp.float32),
            pltpu.VMEM((keys, rows), jnp.float32),
        ],
        compiler_params=pltpu.CompilerParams(vmem_limit_bytes=16 << 20),
        cost_estimate=pl.CostEstimate(
            flops=16 * TREE * keys * width, bytes_accessed=3 << 20, transcendentals=0
        ),
    )(live, sinks, queries, tree_k, tree_v, cache_k, cache_v, bias)


def project_kernel(blocks, requests, parts, start, ranks, final, whom_ref, *refs):
    weights, refs = refs[:blocks], refs[blocks:]
    attention, refs = refs[: requests * parts], refs[requests * parts :]
    outs, (held, sems) = refs[:-2], refs[-2:]
    base_ref = None
    if final and start:
        base_ref, *outs = outs
    depth = attention[0].shape[0]
    lanes = slice(start * depth, (start + parts) * depth)
    copies = [
        pltpu.make_async_copy(block.at[:, lanes], held.at[n], sems.at[n])
        for n, block in enumerate(weights)
    ]
    for copy in copies:
        copy.start()
    rank, rows = whom_ref[1], outs[0].shape[-1]
    for n, copy in enumerate(copies):
        copy.wait()
        for which in range(requests):
            for shift, out_ref in enumerate(outs):
                span = slice(None)
                if len(outs) > 1:
                    span = pl.ds(pl.multiple_of((rank + shift) % ranks * rows, rows), rows)
                total = 0.0 if base_ref is None else base_ref[which, n, :, span]
                for part in range(parts):
                    chunk = attention[which * parts + part]
                    block = held[n, :, part * depth : (part + 1) * depth]
                    total = total + product(block, chunk[:, span])
                out_ref[which, n] = total.astype(out_ref.dtype)


def project(whom, ranks, weights, requests, start=0, final=True, base=None):
    columns, width = weights[0].shape
    chunks = [chunk for request in requests for chunk in request]
    parts = len(requests[0])
    rows = TREE // ranks
    cut = final and rows % 128 == 0
    shape = (len(requests), len(weights), columns, rows if cut else TREE)
    kind = jax.ShapeDtypeStruct(shape, jnp.bfloat16 if final else jnp.float32)
    vmem = pl.BlockSpec(memory_space=pltpu.VMEM)
    count = ranks if cut else 1
    bases = [] if base is None else [base]
    outs = pl.pallas_call(
        functools.partial(
            project_kernel, len(weights), len(requests), parts, start, ranks, final
        ),
        out_shape=[kind] * count,
        in_specs=[pl.BlockSpec(memory_space=pltpu.SMEM)]
        + [pl.BlockSpec(memory_space=pl.ANY)] * len(weights)
        + [vmem] * (len(chunks) + len(bases)),
        out_specs=[vmem] * count,
        scratch_shapes=[
            pltpu.VMEM((len(weights), columns, parts * chunks[0].shape[0]), jnp.bfloat16),
            pltpu.SemaphoreType.DMA((len(weights),)),
        ],
        compiler_params=pltpu.CompilerParams(vmem_limit_bytes=20 << 20),
        cost_estimate=pl.CostEstimate(
            flops=4 * len(weights) * columns * chunks[0].shape[0] * len(chunks) * TREE,
            bytes_accessed=2 * len(weights) * columns * (width + 2 * TREE),
            transcendentals=0,
        ),
    )(whom, *weights, *chunks, *bases)
    if cut or not final:
        return list(outs)
    return [
        lax.dynamic_slice_in_dim(outs[0], (whom[1] + shift) % ranks * rows, rows, 3)
        for shift in range(ranks)
    ]


def settle_kernel(count, *refs):
    for which, out_ref in enumerate(refs[count:]):
        total = refs[0][which].astype(jnp.float32)
        for term in refs[1:count]:
            total = total + term[which].astype(jnp.float32)
        out_ref[...] = total.astype(jnp.bfloat16)


def settle(terms):
    vmem = pl.BlockSpec(memory_space=pltpu.VMEM)
    shape = jax.ShapeDtypeStruct(terms[0].shape[1:], jnp.bfloat16)
    requests = terms[0].shape[0]
    return pl.pallas_call(
        functools.partial(settle_kernel, len(terms)),
        out_shape=[shape] * requests,
        in_specs=[vmem] * len(terms),
        out_specs=[vmem] * requests,
        compiler_params=pltpu.CompilerParams(vmem_limit_bytes=16 << 20),
    )(*terms)


def arrange_kernel(whom_ref, slot_ref, *refs):
    parts, (out_ref, held) = refs[:-2], refs[-2:]
    request = whom_ref[0]
    at = 0
    for part in parts:
        held[at : at + part.shape[0]] = part[...]
        at += part.shape[0]
    slots, columns = at // 2, held.shape[1]

    def block(index):
        slot = slot_ref[request * slots + index // 2]
        return held[slot + jnp.where(request % 2 == index % 2, 0, slots)].astype(jnp.float32)

    for pair in range(slots):
        both = jnp.concatenate([block(2 * pair), block(2 * pair + 1)], 0)
        out_ref[2 * pair * columns : 2 * (pair + 1) * columns] = both.astype(out_ref.dtype)


def arrange(whom, slot_of, mine, other):
    vmem = pl.BlockSpec(memory_space=pltpu.VMEM)
    smem = pl.BlockSpec(memory_space=pltpu.SMEM)
    columns, rows = mine[0].shape[1:]
    parts = mine + other
    count = sum(part.shape[0] for part in parts)
    return pl.pallas_call(
        arrange_kernel,
        out_shape=jax.ShapeDtypeStruct((count * columns, rows), jnp.bfloat16),
        in_specs=[smem, smem] + [vmem] * len(parts),
        out_specs=vmem,
        scratch_shapes=[pltpu.VMEM((count, columns, rows), jnp.bfloat16)],
        compiler_params=pltpu.CompilerParams(vmem_limit_bytes=16 << 20),
        name="arrange",
    )(whom, slot_of, *parts)


def exchange(reqs):
    if reqs != 16:
        half = reqs // 2
        return [
            (0, [(i, (i + 2 * shift) % reqs) for i in range(reqs)]) for shift in range(1, half)
        ]
    outer = [(i, i ^ 4) for i in range(reqs)]
    inner = [(i, i ^ 12 if i // 4 in (1, 2) else i ^ 2) for i in range(reqs)]
    return [(0, outer), (0, inner), (1, inner), (2, outer), (3, outer), (4, inner), (5, inner)]


def slots_of(reqs, moves):
    held = [[i] for i in range(reqs)]
    for slot, hops in moves:
        sent = {there: held[here][slot] for here, there in hops}
        for i in range(reqs):
            held[i].append(sent[i])
    return [held[i].index(2 * j + i % 2) for i in range(reqs) for j in range(reqs // 2)]


def timetable(moves, parts):
    plan = {}
    calls = (0, 2, 5)
    for n in range(len(moves)):
        at = calls[n // 2] if n // 2 < len(calls) else parts
        plan.setdefault(min(at, parts), []).append(n)
    return plan


def per_device(
    reqs,
    ranks,
    tree_queries,
    tree_keys,
    tree_values,
    cache_keys,
    cache_values,
    sinks,
    parents,
    tile_counts,
    out_weight,
):
    whom = jnp.stack([lax.axis_index("req"), lax.axis_index("tp")]).astype(jnp.int32)
    swap = [(i, i ^ 1) for i in range(reqs)]
    moves = exchange(reqs)
    slots = [out_weight.T]

    kv_local = cache_keys.shape[2] // HEAD_DIM
    odd = kv_local % 2 * HEAD_DIM
    pad = ((0, 0), (0, odd))
    local = [jnp.pad(a[0], pad) for a in (tree_keys, tree_values, cache_keys, cache_values)]
    own, partner = [], []
    parts = 2 * kv_local
    plan = timetable(moves, parts)
    live = tile_counts
    whom, parents = lax.optimization_barrier((whom, parents))
    for part in range(parts + 1):
        for n in plan.get(part, []):
            slot, hops = moves[n]
            block = slots[slot]
            if 0 < part < parts:
                block, live = lax.optimization_barrier((block, live))
            slots.append(lax.ppermute(block, "req", hops))
        if part == parts:
            break
        if part == 0:
            bias = ancestry(parents)
        chunk = attend(part, parts, live, sinks[None], tree_queries[0], *local, bias)
        live, chunk = lax.optimization_barrier((live, chunk))
        own.append(chunk)
        partner.append(lax.ppermute(chunk, "req", swap))

    def share(terms):
        for shift in range(1, ranks):
            hops = [(r, (r + shift) % ranks) for r in range(ranks)]
            terms[shift] = lax.ppermute(terms[shift], "tp", hops)
        return settle(terms)

    def multiply(weights, requests, **how):
        return project(whom, ranks, weights, requests, **how)

    early, late = slots[:-1], slots[-1:]
    (base,) = multiply(early, [partner[:-1]], final=False)
    last = multiply(early, [partner[-1:]], start=parts - 1, base=base)
    (given,) = share(last)
    other = [lax.ppermute(given, "req", swap)]
    mine = []
    for weights in (early[:2], early[2:]):
        mine += share(multiply(weights, [own]))
    kept, given = share(multiply(late, [own, partner]))
    mine.append(kept)
    other.append(lax.ppermute(given, "req", swap))
    slot_of = jnp.asarray(slots_of(reqs, moves), jnp.int32)
    return arrange(whom, slot_of, mine, other).T[None]


def solution(mesh):
    in_specs = (
        P("req", None, "tp"),
        P("req", None, "tp"),
        P("req", None, "tp"),
        P("req", None, "tp"),
        P("req", None, "tp"),
        P("tp"),
        P("req", None),
        P("req"),
        P("tp", "req"),
    )
    out_specs = P("req", "tp", None)
    return jax.shard_map(
        functools.partial(per_device, mesh.shape["req"], mesh.shape["tp"]),
        mesh=mesh,
        in_specs=in_specs,
        out_specs=out_specs,
        check_vma=False,
    )
```

```python
import functools

import jax
import jax.numpy as jnp
from jax import lax
from jax.experimental import pallas as pl
from jax.experimental.pallas import tpu as pltpu
from jax.sharding import PartitionSpec as P


HEADS = 64
KV_HEADS = 8
HEAD_DIM = 64
TREE = 512
TILE = 128
WIDE = 2 * HEAD_DIM
LOG2_E = 1.4426950408889634
masked_score = -1e30


def product(left, right):
    return jnp.dot(left, right, preferred_element_type=jnp.float32)


def ancestry_kernel(parent_ref, bias_ref, seen):
    tiles = TREE // TILE
    lane = lax.broadcasted_iota(jnp.int32, (TILE, TILE), 1)
    key = lax.broadcasted_iota(jnp.int32, (TILE, TILE), 0)

    def hop(key_tile, row_tile):
        parent = parent_ref[:, row_tile * TILE : (row_tile + 1) * TILE]
        return jnp.broadcast_to(parent, (TILE, TILE)) == key + key_tile * TILE

    inner = [(hop(t, t) | (lane == key)).astype(jnp.bfloat16) for t in range(tiles)]
    reach = 1
    while reach < TILE:
        inner = [jnp.minimum(product(r, r), 1.0).astype(jnp.bfloat16) for r in inner]
        reach *= 2
    seen[...] = jnp.zeros_like(seen)
    for t in range(tiles):
        rows = slice(t * TILE, (t + 1) * TILE)
        if t:
            up = jnp.concatenate([hop(u, t).astype(jnp.bfloat16) for u in range(t)], 0)
            last = product(up, inner[t]).astype(jnp.bfloat16)
            seen[: t * TILE, rows] = product(seen[: t * TILE, : t * TILE], last).astype(jnp.bfloat16)
        seen[rows, rows] = inner[t]
    bias_ref[...] = jnp.where(seen[...].astype(jnp.float32) > 0.5, 0.0, masked_score)


def ancestry(parents):
    return pl.pallas_call(
        ancestry_kernel,
        out_shape=jax.ShapeDtypeStruct((TREE, TREE), jnp.float32),
        in_specs=[pl.BlockSpec(memory_space=pltpu.VMEM)],
        out_specs=pl.BlockSpec(memory_space=pltpu.VMEM),
        scratch_shapes=[pltpu.VMEM((TREE, TREE), jnp.bfloat16)],
        compiler_params=pltpu.CompilerParams(vmem_limit_bytes=8 << 20),
        name="ancestry",
        cost_estimate=pl.CostEstimate(
            flops=80 * TREE**3, bytes_accessed=4 * TREE * TREE, transcendentals=0
        ),
    )(parents)


ONES = 16


def attend_kernel(
    kv_head,
    first,
    live_ref,
    sink_ref,
    query_ref,
    tree_k_ref,
    tree_v_ref,
    cache_k_ref,
    cache_v_ref,
    bias_ref,
    out_ref,
    key_left,
    key_right,
    values,
    score_left,
    score_right,
):
    ctx = cache_k_ref.shape[0]
    pairs = out_ref.shape[0] // WIDE
    factor = LOG2_E * HEAD_DIM**-0.5
    sink_scale = HEAD_DIM**0.5
    near = kv_head % 2
    columns = slice(kv_head // 2 * WIDE, kv_head // 2 * WIDE + WIDE)
    for start, key_src, value_src in (
        (0, cache_k_ref, cache_v_ref),
        (ctx, tree_k_ref, tree_v_ref),
    ):
        rows = key_src.shape[0]
        span = slice(start, start + rows)
        right = lax.broadcasted_iota(jnp.int32, (rows, WIDE), 1) >= HEAD_DIM
        own = right if near else jnp.logical_not(right)
        key = jnp.where(own, key_src[:, columns].astype(jnp.float32), 0.0)
        moved = pltpu.roll(key, HEAD_DIM, 1)
        key_left[span] = (moved if near else key).astype(jnp.bfloat16)
        key_right[span] = (key if near else moved).astype(jnp.bfloat16)
        turned = value_src[:, columns].astype(jnp.float32).T
        values[:HEAD_DIM, span] = turned[near * HEAD_DIM : (near + 1) * HEAD_DIM].astype(jnp.bfloat16)
    values[HEAD_DIM:] = jnp.ones((ONES, values.shape[1]), jnp.bfloat16)
    live = live_ref[0]

    def score(tile, keys, store):
        rows = pl.ds(pl.multiple_of(tile * TILE, TILE), TILE)
        start = first * HEAD_DIM
        query = jnp.concatenate(
            [query_ref[rows, start + p * WIDE : start + (p + 1) * WIDE] for p in range(pairs)], 0
        )
        store[...] = lax.dot_general(
            keys[...], query, (((1,), (1,)), ((), ())), preferred_element_type=jnp.float32
        )

    def mix(tile, side, store):
        rows = pl.ds(pl.multiple_of(tile * TILE, TILE), TILE)
        step = 256
        total_keys = store.shape[0]
        peak = None
        for at in range(0, total_keys, step):
            part = store[at : at + step]
            if at >= ctx:
                bias = bias_ref[at - ctx : at - ctx + step, rows]
                part = part + jnp.concatenate([bias] * pairs, 1)
                store[at : at + step] = part
            high = part.max(0, keepdims=True)
            peak = high if peak is None else jnp.maximum(peak, high)
        sinks = [sink_ref[:, first + 2 * p + side : first + 2 * p + side + 1] for p in range(pairs)]
        sink = jnp.concatenate([jnp.broadcast_to(s, (1, TILE)) for s in sinks], 1) * sink_scale
        peak = jnp.maximum(peak, sink)
        sums = 0.0
        for at in range(0, total_keys, step):
            probs = jnp.exp2((store[at : at + step] - peak) * factor).astype(jnp.bfloat16)
            sums = sums + product(values[:, at : at + step], probs)
        below = sums[HEAD_DIM : HEAD_DIM + 1] + jnp.exp2((sink - peak) * factor)
        mixed = (sums[:HEAD_DIM] / below).astype(out_ref.dtype)
        for p in range(pairs):
            top = p * WIDE + side * HEAD_DIM
            out_ref[top : top + HEAD_DIM, rows] = mixed[:, p * TILE : (p + 1) * TILE]

    out_ref[...] = jnp.zeros_like(out_ref)
    score(0, key_left, score_left)

    @pl.loop(0, live)
    def tile_step(tile):
        score(tile, key_right, score_right)
        mix(tile, 0, score_left)
        score(jnp.minimum(tile + 1, live - 1), key_left, score_left)
        mix(tile, 1, score_right)


def attend(part, parts, live, sinks, queries, tree_k, tree_v, cache_k, cache_v, bias):
    width = queries.shape[1] // parts
    first = part * width // HEAD_DIM
    kv_head = first // (HEADS // KV_HEADS)
    keys = cache_k.shape[0] + tree_k.shape[0]
    smem = pl.BlockSpec(memory_space=pltpu.SMEM)
    vmem = pl.BlockSpec(memory_space=pltpu.VMEM)
    rows = width // WIDE * TILE
    return pl.pallas_call(
        functools.partial(attend_kernel, kv_head, first),
        out_shape=jax.ShapeDtypeStruct((width, TREE), jnp.bfloat16),
        in_specs=[smem] + [vmem] * 7,
        out_specs=vmem,
        scratch_shapes=[
            pltpu.VMEM((keys, WIDE), jnp.bfloat16),
            pltpu.VMEM((keys, WIDE), jnp.bfloat16),
            pltpu.VMEM((HEAD_DIM + ONES, keys), jnp.bfloat16),
            pltpu.VMEM((keys, rows), jnp.float32),
            pltpu.VMEM((keys, rows), jnp.float32),
        ],
        compiler_params=pltpu.CompilerParams(vmem_limit_bytes=16 << 20),
        cost_estimate=pl.CostEstimate(
            flops=16 * TREE * keys * width, bytes_accessed=3 << 20, transcendentals=0
        ),
    )(live, sinks, queries, tree_k, tree_v, cache_k, cache_v, bias)


def project_kernel(pieces, requests, parts, start, skip, ranks, final, whom_ref, *refs):
    weights, refs = refs[: sum(pieces)], refs[sum(pieces) :]
    attention, refs = refs[: requests * parts], refs[requests * parts :]
    outs, (held, sems) = refs[:-2], refs[-2:]
    base_ref = None
    if final and start:
        base_ref, *outs = outs
    depth = attention[0].shape[0]
    lanes = slice(start * depth, (start + parts) * depth)
    copies = []
    for n, count in enumerate(pieces):
        block = weights[sum(pieces[:n]) : sum(pieces[: n + 1])]
        if count == 1:
            copies.append([pltpu.make_async_copy(block[0].at[:, lanes], held.at[n], sems.at[n, 0])])
            continue
        width = block[0].shape[1]
        copies.append(
            [
                pltpu.make_async_copy(
                    piece, held.at[n, :, i * width : (i + 1) * width], sems.at[n, i]
                )
                for i, piece in enumerate(block)
            ]
        )
    for copy in sum(copies, []):
        copy.start()
    rank, rows = whom_ref[1], outs[0].shape[-1]
    for n, group in enumerate(copies):
        for copy in group:
            copy.wait()
        for which in range(requests):
            for shift, out_ref in enumerate(outs):
                span = slice(None)
                if len(outs) > 1:
                    span = pl.ds(pl.multiple_of((rank + shift) % ranks * rows, rows), rows)
                total = 0.0 if base_ref is None else base_ref[which, skip + n, :, span]
                for part in range(parts):
                    chunk = attention[which * parts + part]
                    block = held[n, :, part * depth : (part + 1) * depth]
                    total = total + product(block, chunk[:, span])
                out_ref[which, n] = total.astype(out_ref.dtype)


def project(whom, ranks, weights, requests, start=0, final=True, base=None, skip=0):
    blocks = [block if isinstance(block, tuple) else (block,) for block in weights]
    pieces = [piece for block in blocks for piece in block]
    columns = pieces[0].shape[0]
    width = sum(piece.shape[1] for piece in blocks[0])
    chunks = [chunk for request in requests for chunk in request]
    parts = len(requests[0])
    rows = TREE // ranks
    cut = final and rows % 128 == 0
    shape = (len(requests), len(weights), columns, rows if cut else TREE)
    kind = jax.ShapeDtypeStruct(shape, jnp.bfloat16 if final else jnp.float32)
    vmem = pl.BlockSpec(memory_space=pltpu.VMEM)
    count = ranks if cut else 1
    bases = [] if base is None else [base]
    outs = pl.pallas_call(
        functools.partial(
            project_kernel,
            [len(block) for block in blocks],
            len(requests),
            parts,
            start,
            skip,
            ranks,
            final,
        ),
        out_shape=[kind] * count,
        in_specs=[pl.BlockSpec(memory_space=pltpu.SMEM)]
        + [pl.BlockSpec(memory_space=pl.ANY)] * len(pieces)
        + [vmem] * (len(chunks) + len(bases)),
        out_specs=[vmem] * count,
        scratch_shapes=[
            pltpu.VMEM((len(weights), columns, parts * chunks[0].shape[0]), jnp.bfloat16),
            pltpu.SemaphoreType.DMA((len(weights), max(map(len, blocks)))),
        ],
        compiler_params=pltpu.CompilerParams(vmem_limit_bytes=20 << 20),
        cost_estimate=pl.CostEstimate(
            flops=4 * len(weights) * columns * chunks[0].shape[0] * len(chunks) * TREE,
            bytes_accessed=2 * len(weights) * columns * (width + 2 * TREE),
            transcendentals=0,
        ),
    )(whom, *pieces, *chunks, *bases)
    if cut or not final:
        return list(outs)
    return [
        lax.dynamic_slice_in_dim(outs[0], (whom[1] + shift) % ranks * rows, rows, 3)
        for shift in range(ranks)
    ]


def halve_kernel(low_ref, high_ref, low_half, high_half, sems):
    width = low_half.shape[1]
    low = pltpu.make_async_copy(low_ref.at[:, :width], low_half, sems.at[0])
    high = pltpu.make_async_copy(high_ref.at[:, width:], high_half, sems.at[1])
    low.start()
    high.start()
    low.wait()
    high.wait()


def halve(low, high):
    half = jax.ShapeDtypeStruct((low.shape[0], low.shape[1] // 2), low.dtype)
    return pl.pallas_call(
        halve_kernel,
        out_shape=[half] * 2,
        in_specs=[pl.BlockSpec(memory_space=pl.ANY)] * 2,
        out_specs=[pl.BlockSpec(memory_space=pltpu.VMEM)] * 2,
        scratch_shapes=[pltpu.SemaphoreType.DMA((2,))],
        compiler_params=pltpu.CompilerParams(vmem_limit_bytes=8 << 20),
        name="halve",
    )(low, high)


def settle_kernel(count, *refs):
    for which, out_ref in enumerate(refs[count:]):
        total = refs[0][which].astype(jnp.float32)
        for term in refs[1:count]:
            total = total + term[which].astype(jnp.float32)
        out_ref[...] = total.astype(jnp.bfloat16)


def settle(terms):
    vmem = pl.BlockSpec(memory_space=pltpu.VMEM)
    shape = jax.ShapeDtypeStruct(terms[0].shape[1:], jnp.bfloat16)
    requests = terms[0].shape[0]
    return pl.pallas_call(
        functools.partial(settle_kernel, len(terms)),
        out_shape=[shape] * requests,
        in_specs=[vmem] * len(terms),
        out_specs=[vmem] * requests,
        compiler_params=pltpu.CompilerParams(vmem_limit_bytes=16 << 20),
    )(*terms)


def arrange_kernel(whom_ref, slot_ref, *refs):
    parts, (out_ref, held) = refs[:-2], refs[-2:]
    request = whom_ref[0]
    at = 0
    for part in parts:
        held[at : at + part.shape[0]] = part[...]
        at += part.shape[0]
    slots, columns = at // 2, held.shape[1]

    def block(index):
        slot = slot_ref[request * slots + index // 2]
        return held[slot + jnp.where(request % 2 == index % 2, 0, slots)].astype(jnp.float32)

    for pair in range(slots):
        both = jnp.concatenate([block(2 * pair), block(2 * pair + 1)], 0)
        out_ref[2 * pair * columns : 2 * (pair + 1) * columns] = both.astype(out_ref.dtype)


def arrange(whom, slot_of, mine, other):
    vmem = pl.BlockSpec(memory_space=pltpu.VMEM)
    smem = pl.BlockSpec(memory_space=pltpu.SMEM)
    columns, rows = mine[0].shape[1:]
    parts = mine + other
    count = sum(part.shape[0] for part in parts)
    return pl.pallas_call(
        arrange_kernel,
        out_shape=jax.ShapeDtypeStruct((count * columns, rows), jnp.bfloat16),
        in_specs=[smem, smem] + [vmem] * len(parts),
        out_specs=vmem,
        scratch_shapes=[pltpu.VMEM((count, columns, rows), jnp.bfloat16)],
        compiler_params=pltpu.CompilerParams(vmem_limit_bytes=16 << 20),
        name="arrange",
    )(whom, slot_of, *parts)


def exchange(reqs):
    if reqs != 16:
        half = reqs // 2
        return [
            (0, [(i, (i + 2 * shift) % reqs) for i in range(reqs)]) for shift in range(1, half)
        ]
    outer = [(i, i ^ 4) for i in range(reqs)]
    inner = [(i, i ^ 12 if i // 4 in (1, 2) else i ^ 2) for i in range(reqs)]
    return [
        (0, outer),
        (0, inner),
        (1, inner),
        (2, outer),
        (3, outer),
        (4, inner),
        ((5, 6), (inner, outer)),
    ]


def slots_of(reqs, moves):
    held = [[i] for i in range(reqs)]
    for slot, hops in moves:
        if isinstance(slot, tuple):
            slot, hops = slot[0], hops[0]
        sent = {there: held[here][slot] for here, there in hops}
        for i in range(reqs):
            held[i].append(sent[i])
    return [held[i].index(2 * j + i % 2) for i in range(reqs) for j in range(reqs // 2)]


def timetable(moves, parts):
    plan = {}
    calls = (0, 3, 6)
    for n in range(len(moves)):
        at = calls[n // 2] if n // 2 < len(calls) else parts + 1
        plan.setdefault(min(at, parts + 1), []).append(n)
    return plan


def per_device(
    reqs,
    ranks,
    tree_queries,
    tree_keys,
    tree_values,
    cache_keys,
    cache_values,
    sinks,
    parents,
    tile_counts,
    out_weight,
):
    whom = jnp.stack([lax.axis_index("req"), lax.axis_index("tp")]).astype(jnp.int32)
    swap = [(i, i ^ 1) for i in range(reqs)]
    moves = exchange(reqs)
    slots = [out_weight.T]

    kv_local = cache_keys.shape[2] // HEAD_DIM
    odd = kv_local % 2 * HEAD_DIM
    pad = ((0, 0), (0, odd))
    local = [jnp.pad(a[0], pad) for a in (tree_keys, tree_values, cache_keys, cache_values)]
    own, partner = [], []
    parts = 2 * kv_local
    plan = timetable(moves, parts)
    live = tile_counts
    whom, parents = lax.optimization_barrier((whom, parents))
    for part in range(parts + 1):
        for n in plan.get(part, []):
            slot, hops = moves[n]
            block = slots[slot]
            if part:
                block, live = lax.optimization_barrier((block, live))
            slots.append(lax.ppermute(block, "req", hops))
        if part == parts:
            break
        if part == 0:
            bias = ancestry(parents)
        chunk = attend(part, parts, live, sinks[None], tree_queries[0], *local, bias)
        live, chunk = lax.optimization_barrier((live, chunk))
        own.append(chunk)
        partner.append(lax.ppermute(chunk, "req", swap))

    def share(terms):
        for shift in range(1, ranks):
            hops = [(r, (r + shift) % ranks) for r in range(ranks)]
            terms[shift] = lax.ppermute(terms[shift], "tp", hops)
        return settle(terms)

    def multiply(weights, requests, **how):
        return project(whom, ranks, weights, requests, **how)

    early = slots[:5]
    (base,) = multiply(early, [partner[:-1]], final=False)
    for n in plan.get(parts + 1, []):
        slot, hops = moves[n]
        if isinstance(slot, tuple):
            low, high, base = lax.optimization_barrier((slots[slot[0]], slots[slot[1]], base))
            halves = halve(low, high)
            halves = [lax.ppermute(h, "req", hop) for h, hop in zip(halves, hops)]
            slots.append(tuple(halves))
            continue
        block, base = lax.optimization_barrier((slots[slot], base))
        slots.append(lax.ppermute(block, "req", hops))
    mine, other = [], []
    for span in (slice(0, 2), slice(2, None)):
        ready = multiply(early[span], [partner[-1:]], start=parts - 1, base=base, skip=span.start)
        (given,) = share(ready)
        other.append(lax.ppermute(given, "req", swap))
    for late in (slots[len(early) : -1], slots[-1:]):
        kept, given = share(multiply(late, [own, partner]))
        mine.append(kept)
        other.append(lax.ppermute(given, "req", swap))
    owned = [*share(multiply(early[:2], [own])), *share(multiply(early[2:], [own]))]
    mine = owned + mine
    slot_of = jnp.asarray(slots_of(reqs, moves), jnp.int32)
    return arrange(whom, slot_of, mine, other).T[None]


def solution(mesh):
    in_specs = (
        P("req", None, "tp"),
        P("req", None, "tp"),
        P("req", None, "tp"),
        P("req", None, "tp"),
        P("req", None, "tp"),
        P("tp"),
        P("req", None),
        P("req"),
        P("tp", "req"),
    )
    out_specs = P("req", "tp", None)
    return jax.shard_map(
        functools.partial(per_device, mesh.shape["req"], mesh.shape["tp"]),
        mesh=mesh,
        in_specs=in_specs,
        out_specs=out_specs,
        check_vma=False,
    )
```

```python
import functools

import jax
import jax.numpy as jnp
from jax import lax
from jax.experimental import pallas as pl
from jax.experimental.pallas import tpu as pltpu
from jax.sharding import PartitionSpec as P


HEADS = 64
KV_HEADS = 8
HEAD_DIM = 64
TREE = 512
TILE = 128
WIDE = 2 * HEAD_DIM
LOG2_E = 1.4426950408889634
masked_score = -1e30


def product(left, right):
    return jnp.dot(left, right, preferred_element_type=jnp.float32)


def ancestry_kernel(parent_ref, bias_ref, seen):
    tiles = TREE // TILE
    lane = lax.broadcasted_iota(jnp.int32, (TILE, TILE), 1)
    key = lax.broadcasted_iota(jnp.int32, (TILE, TILE), 0)

    def hop(key_tile, row_tile):
        parent = parent_ref[:, row_tile * TILE : (row_tile + 1) * TILE]
        return jnp.broadcast_to(parent, (TILE, TILE)) == key + key_tile * TILE

    inner = [(hop(t, t) | (lane == key)).astype(jnp.bfloat16) for t in range(tiles)]
    reach = 1
    while reach < TILE:
        inner = [jnp.minimum(product(r, r), 1.0).astype(jnp.bfloat16) for r in inner]
        reach *= 2
    seen[...] = jnp.zeros_like(seen)
    for t in range(tiles):
        rows = slice(t * TILE, (t + 1) * TILE)
        if t:
            up = jnp.concatenate([hop(u, t).astype(jnp.bfloat16) for u in range(t)], 0)
            last = product(up, inner[t]).astype(jnp.bfloat16)
            seen[: t * TILE, rows] = product(seen[: t * TILE, : t * TILE], last).astype(jnp.bfloat16)
        seen[rows, rows] = inner[t]
    bias_ref[...] = jnp.where(seen[...].astype(jnp.float32) > 0.5, 0.0, masked_score)


def ancestry(parents):
    return pl.pallas_call(
        ancestry_kernel,
        out_shape=jax.ShapeDtypeStruct((TREE, TREE), jnp.float32),
        in_specs=[pl.BlockSpec(memory_space=pltpu.VMEM)],
        out_specs=pl.BlockSpec(memory_space=pltpu.VMEM),
        scratch_shapes=[pltpu.VMEM((TREE, TREE), jnp.bfloat16)],
        compiler_params=pltpu.CompilerParams(vmem_limit_bytes=8 << 20),
        name="ancestry",
        cost_estimate=pl.CostEstimate(
            flops=80 * TREE**3, bytes_accessed=4 * TREE * TREE, transcendentals=0
        ),
    )(parents)


ONES = 16


def attend_kernel(
    kv_head,
    first,
    live_ref,
    sink_ref,
    query_ref,
    tree_k_ref,
    tree_v_ref,
    cache_k_ref,
    cache_v_ref,
    bias_ref,
    out_ref,
    key_left,
    key_right,
    values,
    score_left,
    score_right,
):
    ctx = cache_k_ref.shape[0]
    pairs = out_ref.shape[0] // WIDE
    factor = LOG2_E * HEAD_DIM**-0.5
    sink_scale = HEAD_DIM**0.5
    near = kv_head % 2
    columns = slice(kv_head // 2 * WIDE, kv_head // 2 * WIDE + WIDE)
    for start, key_src, value_src in (
        (0, cache_k_ref, cache_v_ref),
        (ctx, tree_k_ref, tree_v_ref),
    ):
        rows = key_src.shape[0]
        span = slice(start, start + rows)
        right = lax.broadcasted_iota(jnp.int32, (rows, WIDE), 1) >= HEAD_DIM
        own = right if near else jnp.logical_not(right)
        key = jnp.where(own, key_src[:, columns].astype(jnp.float32), 0.0)
        moved = pltpu.roll(key, HEAD_DIM, 1)
        key_left[span] = (moved if near else key).astype(jnp.bfloat16)
        key_right[span] = (key if near else moved).astype(jnp.bfloat16)
        turned = value_src[:, columns].astype(jnp.float32).T
        values[:HEAD_DIM, span] = turned[near * HEAD_DIM : (near + 1) * HEAD_DIM].astype(jnp.bfloat16)
    values[HEAD_DIM:] = jnp.ones((ONES, values.shape[1]), jnp.bfloat16)
    live = live_ref[0]

    def score(tile, keys, store):
        rows = pl.ds(pl.multiple_of(tile * TILE, TILE), TILE)
        start = first * HEAD_DIM
        query = jnp.concatenate(
            [query_ref[rows, start + p * WIDE : start + (p + 1) * WIDE] for p in range(pairs)], 0
        )
        store[...] = lax.dot_general(
            keys[...], query, (((1,), (1,)), ((), ())), preferred_element_type=jnp.float32
        )

    def mix(tile, side, store):
        rows = pl.ds(pl.multiple_of(tile * TILE, TILE), TILE)
        step = 256
        total_keys = store.shape[0]
        peak = None
        for at in range(0, total_keys, step):
            part = store[at : at + step]
            if at >= ctx:
                bias = bias_ref[at - ctx : at - ctx + step, rows]
                part = part + jnp.concatenate([bias] * pairs, 1)
                store[at : at + step] = part
            high = part.max(0, keepdims=True)
            peak = high if peak is None else jnp.maximum(peak, high)
        sinks = [sink_ref[:, first + 2 * p + side : first + 2 * p + side + 1] for p in range(pairs)]
        sink = jnp.concatenate([jnp.broadcast_to(s, (1, TILE)) for s in sinks], 1) * sink_scale
        peak = jnp.maximum(peak, sink)
        sums = 0.0
        for at in range(0, total_keys, step):
            probs = jnp.exp2((store[at : at + step] - peak) * factor).astype(jnp.bfloat16)
            sums = sums + product(values[:, at : at + step], probs)
        below = sums[HEAD_DIM : HEAD_DIM + 1] + jnp.exp2((sink - peak) * factor)
        mixed = (sums[:HEAD_DIM] / below).astype(out_ref.dtype)
        for p in range(pairs):
            top = p * WIDE + side * HEAD_DIM
            out_ref[top : top + HEAD_DIM, rows] = mixed[:, p * TILE : (p + 1) * TILE]

    out_ref[...] = jnp.zeros_like(out_ref)
    score(0, key_left, score_left)

    @pl.loop(0, live - 1)
    def tile_step(tile):
        score(tile, key_right, score_right)
        mix(tile, 0, score_left)
        score(tile + 1, key_left, score_left)
        mix(tile, 1, score_right)

    score(live - 1, key_right, score_right)
    mix(live - 1, 0, score_left)
    mix(live - 1, 1, score_right)


def attend(part, parts, live, sinks, queries, tree_k, tree_v, cache_k, cache_v, bias):
    width = queries.shape[1] // parts
    first = part * width // HEAD_DIM
    kv_head = first // (HEADS // KV_HEADS)
    keys = cache_k.shape[0] + tree_k.shape[0]
    smem = pl.BlockSpec(memory_space=pltpu.SMEM)
    vmem = pl.BlockSpec(memory_space=pltpu.VMEM)
    rows = width // WIDE * TILE
    return pl.pallas_call(
        functools.partial(attend_kernel, kv_head, first),
        out_shape=jax.ShapeDtypeStruct((width, TREE), jnp.bfloat16),
        in_specs=[smem] + [vmem] * 7,
        out_specs=vmem,
        scratch_shapes=[
            pltpu.VMEM((keys, WIDE), jnp.bfloat16),
            pltpu.VMEM((keys, WIDE), jnp.bfloat16),
            pltpu.VMEM((HEAD_DIM + ONES, keys), jnp.bfloat16),
            pltpu.VMEM((keys, rows), jnp.float32),
            pltpu.VMEM((keys, rows), jnp.float32),
        ],
        compiler_params=pltpu.CompilerParams(vmem_limit_bytes=16 << 20),
        cost_estimate=pl.CostEstimate(
            flops=16 * TREE * keys * width, bytes_accessed=3 << 20, transcendentals=0
        ),
    )(live, sinks, queries, tree_k, tree_v, cache_k, cache_v, bias)


def project_kernel(pieces, requests, parts, start, skip, ranks, final, whom_ref, *refs):
    weights, refs = refs[: sum(pieces)], refs[sum(pieces) :]
    attention, refs = refs[: requests * parts], refs[requests * parts :]
    outs, (held, sems) = refs[:-2], refs[-2:]
    base_ref = None
    if final and start:
        base_ref, *outs = outs
    depth = attention[0].shape[0]
    lanes = slice(start * depth, (start + parts) * depth)
    copies = []
    for n, count in enumerate(pieces):
        block = weights[sum(pieces[:n]) : sum(pieces[: n + 1])]
        if count == 1:
            copies.append([pltpu.make_async_copy(block[0].at[:, lanes], held.at[n], sems.at[n, 0])])
            continue
        width = block[0].shape[1]
        copies.append(
            [
                pltpu.make_async_copy(
                    piece, held.at[n, :, i * width : (i + 1) * width], sems.at[n, i]
                )
                for i, piece in enumerate(block)
            ]
        )
    for copy in sum(copies, []):
        copy.start()
    rank, rows = whom_ref[1], outs[0].shape[-1]
    for n, group in enumerate(copies):
        for copy in group:
            copy.wait()
        for which in range(requests):
            for shift, out_ref in enumerate(outs):
                span = slice(None)
                if len(outs) > 1:
                    span = pl.ds(pl.multiple_of((rank + shift) % ranks * rows, rows), rows)
                total = 0.0 if base_ref is None else base_ref[which, skip + n, :, span]
                for part in range(parts):
                    chunk = attention[which * parts + part]
                    block = held[n, :, part * depth : (part + 1) * depth]
                    total = total + product(block, chunk[:, span])
                out_ref[which, n] = total.astype(out_ref.dtype)


def project(whom, ranks, weights, requests, start=0, final=True, base=None, skip=0):
    blocks = [block if isinstance(block, tuple) else (block,) for block in weights]
    pieces = [piece for block in blocks for piece in block]
    columns = pieces[0].shape[0]
    width = sum(piece.shape[1] for piece in blocks[0])
    chunks = [chunk for request in requests for chunk in request]
    parts = len(requests[0])
    rows = TREE // ranks
    cut = final and rows % 128 == 0
    shape = (len(requests), len(weights), columns, rows if cut else TREE)
    kind = jax.ShapeDtypeStruct(shape, jnp.bfloat16 if final else jnp.float32)
    vmem = pl.BlockSpec(memory_space=pltpu.VMEM)
    count = ranks if cut else 1
    bases = [] if base is None else [base]
    outs = pl.pallas_call(
        functools.partial(
            project_kernel,
            [len(block) for block in blocks],
            len(requests),
            parts,
            start,
            skip,
            ranks,
            final,
        ),
        out_shape=[kind] * count,
        in_specs=[pl.BlockSpec(memory_space=pltpu.SMEM)]
        + [pl.BlockSpec(memory_space=pl.ANY)] * len(pieces)
        + [vmem] * (len(chunks) + len(bases)),
        out_specs=[vmem] * count,
        scratch_shapes=[
            pltpu.VMEM((len(weights), columns, parts * chunks[0].shape[0]), jnp.bfloat16),
            pltpu.SemaphoreType.DMA((len(weights), max(map(len, blocks)))),
        ],
        compiler_params=pltpu.CompilerParams(vmem_limit_bytes=20 << 20),
        cost_estimate=pl.CostEstimate(
            flops=4 * len(weights) * columns * chunks[0].shape[0] * len(chunks) * TREE,
            bytes_accessed=2 * len(weights) * columns * (width + 2 * TREE),
            transcendentals=0,
        ),
    )(whom, *pieces, *chunks, *bases)
    if cut or not final:
        return list(outs)
    return [
        lax.dynamic_slice_in_dim(outs[0], (whom[1] + shift) % ranks * rows, rows, 3)
        for shift in range(ranks)
    ]


def halve_kernel(low_ref, high_ref, low_half, high_half, sems):
    width = low_half.shape[1]
    low = pltpu.make_async_copy(low_ref.at[:, :width], low_half, sems.at[0])
    high = pltpu.make_async_copy(high_ref.at[:, width:], high_half, sems.at[1])
    low.start()
    high.start()
    low.wait()
    high.wait()


def halve(low, high):
    half = jax.ShapeDtypeStruct((low.shape[0], low.shape[1] // 2), low.dtype)
    return pl.pallas_call(
        halve_kernel,
        out_shape=[half] * 2,
        in_specs=[pl.BlockSpec(memory_space=pl.ANY)] * 2,
        out_specs=[pl.BlockSpec(memory_space=pltpu.VMEM)] * 2,
        scratch_shapes=[pltpu.SemaphoreType.DMA((2,))],
        compiler_params=pltpu.CompilerParams(vmem_limit_bytes=8 << 20),
        name="halve",
    )(low, high)


def settle_kernel(count, *refs):
    for which, out_ref in enumerate(refs[count:]):
        total = refs[0][which].astype(jnp.float32)
        for term in refs[1:count]:
            total = total + term[which].astype(jnp.float32)
        out_ref[...] = total.astype(jnp.bfloat16)


def settle(terms):
    vmem = pl.BlockSpec(memory_space=pltpu.VMEM)
    shape = jax.ShapeDtypeStruct(terms[0].shape[1:], jnp.bfloat16)
    requests = terms[0].shape[0]
    return pl.pallas_call(
        functools.partial(settle_kernel, len(terms)),
        out_shape=[shape] * requests,
        in_specs=[vmem] * len(terms),
        out_specs=[vmem] * requests,
        compiler_params=pltpu.CompilerParams(vmem_limit_bytes=16 << 20),
    )(*terms)


def arrange_kernel(whom_ref, slot_ref, *refs):
    parts, (out_ref, held) = refs[:-2], refs[-2:]
    request = whom_ref[0]
    at = 0
    for part in parts:
        held[at : at + part.shape[0]] = part[...]
        at += part.shape[0]
    slots, columns = at // 2, held.shape[1]

    def block(index):
        slot = slot_ref[request * slots + index // 2]
        return held[slot + jnp.where(request % 2 == index % 2, 0, slots)].astype(jnp.float32)

    for pair in range(slots):
        both = jnp.concatenate([block(2 * pair), block(2 * pair + 1)], 0)
        out_ref[2 * pair * columns : 2 * (pair + 1) * columns] = both.astype(out_ref.dtype)


def arrange(whom, slot_of, mine, other):
    vmem = pl.BlockSpec(memory_space=pltpu.VMEM)
    smem = pl.BlockSpec(memory_space=pltpu.SMEM)
    columns, rows = mine[0].shape[1:]
    parts = mine + other
    count = sum(part.shape[0] for part in parts)
    return pl.pallas_call(
        arrange_kernel,
        out_shape=jax.ShapeDtypeStruct((count * columns, rows), jnp.bfloat16),
        in_specs=[smem, smem] + [vmem] * len(parts),
        out_specs=vmem,
        scratch_shapes=[pltpu.VMEM((count, columns, rows), jnp.bfloat16)],
        compiler_params=pltpu.CompilerParams(vmem_limit_bytes=16 << 20),
        name="arrange",
    )(whom, slot_of, *parts)


def exchange(reqs):
    if reqs != 16:
        half = reqs // 2
        return [
            (0, [(i, (i + 2 * shift) % reqs) for i in range(reqs)]) for shift in range(1, half)
        ]
    outer = [(i, i ^ 4) for i in range(reqs)]
    inner = [(i, i ^ 12 if i // 4 in (1, 2) else i ^ 2) for i in range(reqs)]
    return [
        (0, outer),
        (0, inner),
        (1, inner),
        (2, outer),
        (3, outer),
        (4, inner),
        ((5, 6), (inner, outer)),
    ]


def slots_of(reqs, moves):
    held = [[i] for i in range(reqs)]
    for slot, hops in moves:
        if isinstance(slot, tuple):
            slot, hops = slot[0], hops[0]
        sent = {there: held[here][slot] for here, there in hops}
        for i in range(reqs):
            held[i].append(sent[i])
    return [held[i].index(2 * j + i % 2) for i in range(reqs) for j in range(reqs // 2)]


def timetable(moves, parts):
    plan = {}
    calls = (0, 3, 6)
    for n in range(len(moves)):
        at = calls[n // 2] if n // 2 < len(calls) else parts + 1
        plan.setdefault(min(at, parts + 1), []).append(n)
    return plan


def per_device(
    reqs,
    ranks,
    tree_queries,
    tree_keys,
    tree_values,
    cache_keys,
    cache_values,
    sinks,
    parents,
    tile_counts,
    out_weight,
):
    whom = jnp.stack([lax.axis_index("req"), lax.axis_index("tp")]).astype(jnp.int32)
    swap = [(i, i ^ 1) for i in range(reqs)]
    moves = exchange(reqs)
    slots = [out_weight.T]

    kv_local = cache_keys.shape[2] // HEAD_DIM
    odd = kv_local % 2 * HEAD_DIM
    pad = ((0, 0), (0, odd))
    local = [jnp.pad(a[0], pad) for a in (tree_keys, tree_values, cache_keys, cache_values)]
    own, partner = [], []
    parts = 2 * kv_local
    plan = timetable(moves, parts)
    live = tile_counts
    whom, parents = lax.optimization_barrier((whom, parents))
    for part in range(parts + 1):
        for n in plan.get(part, []):
            slot, hops = moves[n]
            block = slots[slot]
            if part:
                block, live = lax.optimization_barrier((block, live))
            slots.append(lax.ppermute(block, "req", hops))
        if part == parts:
            break
        if part == 0:
            bias = ancestry(parents)
        chunk = attend(part, parts, live, sinks[None], tree_queries[0], *local, bias)
        live, chunk = lax.optimization_barrier((live, chunk))
        own.append(chunk)
        partner.append(lax.ppermute(chunk, "req", swap))

    def share(terms):
        for shift in range(1, ranks):
            hops = [(r, (r + shift) % ranks) for r in range(ranks)]
            terms[shift] = lax.ppermute(terms[shift], "tp", hops)
        return settle(terms)

    def multiply(weights, requests, **how):
        return project(whom, ranks, weights, requests, **how)

    early = slots[:5]
    (base,) = multiply(early, [partner[:-1]], final=False)
    for n in plan.get(parts + 1, []):
        slot, hops = moves[n]
        if isinstance(slot, tuple):
            low, high, base = lax.optimization_barrier((slots[slot[0]], slots[slot[1]], base))
            halves = halve(low, high)
            halves = [lax.ppermute(h, "req", hop) for h, hop in zip(halves, hops)]
            slots.append(tuple(halves))
            continue
        block, base = lax.optimization_barrier((slots[slot], base))
        slots.append(lax.ppermute(block, "req", hops))
    mine, other = [], []
    for span in (slice(0, 2), slice(2, None)):
        ready = multiply(early[span], [partner[-1:]], start=parts - 1, base=base, skip=span.start)
        (given,) = share(ready)
        other.append(lax.ppermute(given, "req", swap))
    for late in (slots[len(early) : -1], slots[-1:]):
        kept, given = share(multiply(late, [own, partner]))
        mine.append(kept)
        other.append(lax.ppermute(given, "req", swap))
    owned = [*share(multiply(early[:2], [own])), *share(multiply(early[2:], [own]))]
    mine = owned + mine
    slot_of = jnp.asarray(slots_of(reqs, moves), jnp.int32)
    return arrange(whom, slot_of, mine, other).T[None]


def solution(mesh):
    in_specs = (
        P("req", None, "tp"),
        P("req", None, "tp"),
        P("req", None, "tp"),
        P("req", None, "tp"),
        P("req", None, "tp"),
        P("tp"),
        P("req", None),
        P("req"),
        P("tp", "req"),
    )
    out_specs = P("req", "tp", None)
    return jax.shard_map(
        functools.partial(per_device, mesh.shape["req"], mesh.shape["tp"]),
        mesh=mesh,
        in_specs=in_specs,
        out_specs=out_specs,
        check_vma=False,
    )
```
